32 devices in a mesh: row: 8 (over y, x, core), col: 4 (over z).
Axes of the slice: x: 2, y: 2, z: 4, core: 2. Of those that a mesh axis runs over, the one named last changes fastest.
Arguments:
- sources: float32 [3, 1024, 4096], P(None, 'row', 'col'), may hold values from -32 to 32
- labels: int32 [1024, 4096], P('row', 'col'), may hold values from 0 to 2
Outputs:
- blended: float32 [1024, 4096], P('row', 'col')
- overview_fine: float32 [512, 2048], P('row', 'col')
- overview_mid: float32 [256, 1024], P(None, 'col')
- overview_coarse: float32 [128, 512], P(None, 'col')
The draws below stay inside these ranges and needn't reach their ends.
All inputs are finite; a program needn't handle non-finite values.
Results may differ from the reference program's by a relative error of at most 0.0001.
Values sent between devices are 32-bit elements; how exact they have to be, the bound alone decides.
A program may use at most 64 MiB of HBM per device.

```python
import jax
import jax.numpy as jnp

K = 3
ITERS = 3
H = 1024
W = 4096


def draw_sources(key, part):
    row_frac = jnp.arange(H, dtype=jnp.float32) / H
    col_frac = jnp.arange(W, dtype=jnp.float32) / W
    amplitude = (1.0 + 2.0 * row_frac)[:, None] * (1.0 + 2.0 * col_frac)[None, :] / 3.0
    noise_draw = jnp.clip(jax.random.normal(key, (K, H, W), jnp.float32), -6.0, 6.0)
    return noise_draw * amplitude


def touch_ends(entries, own_key, smallest, top_value):
    place = [jax.random.randint(jax.random.fold_in(own_key, axis), (), 0, length) for axis, length in enumerate(entries.shape)]
    main_axis = entries.shape.index(max(entries.shape))
    neighbour = place[:main_axis] + [(place[main_axis] + 1) % entries.shape[main_axis]] + place[main_axis + 1:]
    return entries.at[tuple(place)].set(smallest).at[tuple(neighbour)].set(top_value)


def setup_inputs(seed: int = 0) -> dict:
    key_of = jax.random.split(jax.random.key(seed), 3)
    return {
        "sources": draw_sources(jax.random.fold_in(key_of[2], 71), 0),
        "labels": touch_ends(jax.random.randint(key_of[1], (H, W), 0, K), jax.random.fold_in(key_of[1], 1), 0, K - 1).astype(jnp.int32),
    }


def apply_stencil(values):
    padded = jnp.pad(values, 1)
    beside = padded[2:, 1:-1] + padded[:-2, 1:-1]
    beside = beside + padded[1:-1, 2:] + padded[1:-1, :-2]
    return 4.0 * values - beside


def average_pool(values):
    return 0.25 * (values[0::2, 0::2] + values[1::2, 0::2] + values[0::2, 1::2] + values[1::2, 1::2])


def reference(sources, labels):
    right_side = jnp.zeros(labels.shape, jnp.float32)
    for channel in range(K):
        right_side = right_side + jnp.where(labels == channel, apply_stencil(sources[channel]), jnp.float32(0.0))
    blended = jnp.zeros(labels.shape, jnp.float32)
    residual = right_side
    direction = right_side
    norm_now = jnp.sum(residual * residual)
    for iteration in range(ITERS):
        applied = apply_stencil(direction)
        step_size = norm_now / jnp.sum(direction * applied)
        blended = blended + step_size * direction
        residual = residual - step_size * applied
        norm_next = jnp.sum(residual * residual)
        direction = residual + (norm_next / norm_now) * direction
        norm_now = norm_next
    overview_fine = average_pool(blended)
    overview_mid = average_pool(overview_fine)
    overview_coarse = average_pool(overview_mid)
    return (blended, overview_fine, overview_mid, overview_coarse)
```

```python
import functools

import jax
import jax.numpy as jnp
from jax import lax
from jax.experimental import pallas as pl
from jax.experimental.pallas import tpu as pltpu
from jax.sharding import PartitionSpec as P

ITERS = 3
MESH = pl.DeviceIdType.MESH
HALO = 4
TOP = 16
SIDES = ((-1, 0), (1, 0), (0, -1), (0, 1), (-1, -1), (-1, 1), (1, -1), (1, 1))


def neighbour_sum(ref, index, start, mid, width):
    above = ref[index + (pl.ds(pl.multiple_of(start - 8, 8), 8), slice(None))]
    below = ref[index + (pl.ds(pl.multiple_of(start + 8, 8), 8), slice(None))]
    sub = lax.broadcasted_iota(jnp.int32, mid.shape, 0)
    up = pltpu.roll(jnp.where(sub == 7, above, mid), 1, axis=0)
    down = pltpu.roll(jnp.where(sub == 0, below, mid), 7, axis=0)
    left = pltpu.roll(mid, 1, axis=1)
    right = pltpu.roll(mid, width - 1, axis=1)
    return (up + down) + (left + right)


def fold_lanes(strip, cols):
    total = strip[:, 0:128]
    for tile in range(1, cols // 128):
        total = total + strip[:, tile * 128:(tile + 1) * 128]
    return total


def quadratic(left, right, moments, shift):
    total = None
    for i, a in enumerate(left):
        for j, b in enumerate(right):
            term = a * b * moments[i + j + shift]
            total = term if total is None else total + term
    return total


def padded_sum(a, b):
    if len(a) < len(b):
        a, b = b, a
    return [x + b[i] if i < len(b) else x for i, x in enumerate(a)]


def coefficients(moments):
    residual = [jnp.ones_like(moments[0])]
    direction = residual
    solution_coords = [jnp.zeros_like(moments[0])]
    norm_now = moments[0]
    for iteration in range(ITERS):
        applied_dot = 4.0 * (
            quadratic(direction, direction, moments, 0)
            - quadratic(direction, direction, moments, 1)
        )
        step = norm_now / applied_dot
        solution_coords = padded_sum(solution_coords, [step * d for d in direction])
        if iteration + 1 < ITERS:
            moved = [-4.0 * step * d for d in direction]
            residual = padded_sum(residual, moved)
            residual = padded_sum(residual, [jnp.zeros_like(step)] + [-m for m in moved])
            norm_next = quadratic(residual, residual, moments, 0)
            ratio = norm_next / norm_now
            direction = padded_sum(residual, [ratio * d for d in direction])
            norm_now = norm_next
    return solution_coords


def kernel(
    n_row, n_col, rows, cols, kinds,
    src_hbm, lab_hbm, blend_ref, fine_ref, mid_ref, coarse_ref,
    src, lab, vec, mask, pack_r, pack_c, got_r, got_c, got_d, moment, mid_all, half,
    load_sem, send_sem, recv_sem, mom_send, mom_recv, mid_send, mid_recv,
):
    width = cols + 128
    n = n_row * n_col
    row, col = lax.axis_index("row"), lax.axis_index("col")
    me = row * n_col + col
    loads = [
        pltpu.make_async_copy(
            src_hbm.at[k], src.at[k, pl.ds(TOP, rows), pl.ds(0, cols)], load_sem.at[k]
        )
        for k in range(kinds)
    ]
    loads.append(
        pltpu.make_async_copy(lab_hbm, lab.at[pl.ds(TOP, rows), pl.ds(0, cols)], load_sem.at[kinds])
    )
    for load in loads:
        load.start()

    barrier = pltpu.get_barrier_semaphore()

    def greet(step, _):
        other = lax.rem(me + step, n)
        pl.semaphore_signal(
            barrier, inc=1, device_id=(other // n_col, lax.rem(other, n_col)), device_id_type=MESH
        )
        return 0

    lax.fori_loop(1, n, greet, 0)

    first_row, last_row = row == 0, row == n_row - 1
    first_col, last_col = col == 0, col == n_col - 1
    quarter = jnp.full((8, width), 0.25, jnp.float32)
    lane = lax.broadcasted_iota(jnp.int32, (8, width), 1)
    off = ((lane >= cols) & (lane < cols + 64) & last_col) | ((lane >= cols + 64) & first_col)
    inside = jnp.where(off, 0.0, quarter)
    mask[0] = jnp.where(first_row, 0.0, inside)
    mask[1] = inside
    mask[2] = jnp.where(last_row, 0.0, inside)
    zero = jnp.zeros((8, width), jnp.float32)
    for which in range(3):
        vec[which, 0:8] = zero
        vec[which, rows + 24:rows + 32] = zero

    for load in loads:
        load.wait()

    for k in range(kinds + 1):
        def edge(rng, lanes):
            if k < kinds:
                return src[k, rng, lanes]
            return lab[rng, lanes].astype(jnp.float32)

        at = slice(HALO * k, HALO * (k + 1))
        pack_r[0, at, :] = edge(pl.ds(TOP, HALO), pl.ds(0, cols))
        pack_r[1, at, :] = edge(pl.ds(TOP + rows - HALO, HALO), pl.ds(0, cols))
    n_pack = HALO * (kinds + 1)
    tile_lane = lax.broadcasted_iota(jnp.int32, (rows, 128), 1)
    packed = jnp.zeros((rows, 128), jnp.float32)
    for k in range(kinds + 1):
        for side in range(2):
            lanes = pl.ds(0 if side == 0 else cols - 128, 128)
            if k < kinds:
                tile = src[k, pl.ds(TOP, rows), lanes]
            else:
                tile = lab[pl.ds(TOP, rows), lanes].astype(jnp.float32)
            target = side * n_pack + HALO * k
            origin = 0 if side == 0 else 128 - HALO
            if (target - origin) % 128:
                tile = pltpu.roll(tile, (target - origin) % 128, axis=1)
            packed = jnp.where((tile_lane >= target) & (tile_lane < target + HALO), tile, packed)
    turned = jnp.transpose(packed)
    pack_c[0] = turned[0:n_pack]
    pack_c[1] = turned[n_pack:2 * n_pack]

    pl.semaphore_wait(barrier, n - 1)

    sends = []
    for i, (dr, dc) in enumerate(SIDES):
        if dc == 0:
            source = pack_r.at[0 if dr < 0 else 1]
            target = got_r.at[1 if dr < 0 else 0]
        elif dr == 0:
            source = pack_c.at[0 if dc < 0 else 1]
            target = got_c.at[1 if dc < 0 else 0]
        else:
            lanes = pl.ds(0 if dc < 0 else cols - 128, 128)
            source = pack_r.at[0 if dr < 0 else 1, :, lanes]
            target = got_d.at[1 if dr < 0 else 0, 1 if dc < 0 else 0]
        there = jnp.logical_and(
            jnp.logical_and(row + dr >= 0, row + dr < n_row),
            jnp.logical_and(col + dc >= 0, col + dc < n_col),
        )
        opposite = SIDES.index((-dr, -dc))
        device = (
            jnp.clip(row + dr, 0, n_row - 1),
            jnp.clip(col + dc, 0, n_col - 1),
        )
        copy = pltpu.make_async_remote_copy(
            src_ref=source, dst_ref=target, send_sem=send_sem.at[i],
            recv_sem=recv_sem.at[opposite], device_id=device, device_id_type=MESH,
        )
        back = pltpu.make_async_remote_copy(
            src_ref=source, dst_ref=got_r.at[0 if dr < 0 else 1] if dc == 0 else (
                got_c.at[0 if dc < 0 else 1] if dr == 0
                else got_d.at[0 if dr < 0 else 1, 0 if dc < 0 else 1]),
            send_sem=send_sem.at[i], recv_sem=recv_sem.at[i],
            device_id=device, device_id_type=MESH,
        )
        sends.append((there, copy, back))
        pl.when(there)(copy.start)
    for there, copy, back in sends:
        pl.when(there)(back.wait_recv)

    halo_lane = lax.broadcasted_iota(jnp.int32, (HALO, 128), 1)
    for side in range(2):
        missing_row = first_row if side == 0 else last_row
        base = TOP - HALO if side == 0 else TOP + rows
        other = TOP - 8 if side == 0 else TOP + rows + HALO
        for k in range(kinds + 1):
            fill = jnp.float32(0.0 if k < kinds else -1.0)
            at = slice(HALO * k, HALO * (k + 1))
            wide = jnp.where(missing_row, fill, got_r[side, at, :])
            right = jnp.where(
                (halo_lane < HALO) & jnp.logical_not(missing_row | last_col),
                got_d[side, 1, at, :], fill)
            corner = jnp.where(
                (halo_lane >= 128 - HALO) & jnp.logical_not(missing_row | first_col),
                got_d[side, 0, at, :], right)
            empty = jnp.full((HALO, width), fill)
            if k < kinds:
                src[k, pl.ds(base, HALO), pl.ds(0, cols)] = wide
                src[k, pl.ds(base, HALO), pl.ds(cols, 128)] = corner
                src[k, pl.ds(other, HALO), :] = empty
            else:
                lab[pl.ds(base, HALO), pl.ds(0, cols)] = wide.astype(jnp.int32)
                lab[pl.ds(base, HALO), pl.ds(cols, 128)] = corner.astype(jnp.int32)
                lab[pl.ds(other, HALO), :] = empty.astype(jnp.int32)
    both = jnp.concatenate(
        [
            got_c[1],
            got_c[0],
            jnp.zeros((128 - 2 * n_pack, rows), jnp.float32),
        ],
        axis=0,
    )
    unturned = jnp.transpose(both)
    for k in range(kinds + 1):
        fill = jnp.float32(0.0 if k < kinds else -1.0)
        right = pltpu.roll(unturned, (-HALO * k) % 128, axis=1)
        left = pltpu.roll(unturned, (128 - HALO - n_pack - HALO * k) % 128, axis=1)
        tile = jnp.where((tile_lane < HALO) & jnp.logical_not(last_col), right, fill)
        tile = jnp.where((tile_lane >= 128 - HALO) & jnp.logical_not(first_col), left, tile)
        if k < kinds:
            src[k, pl.ds(TOP, rows), pl.ds(cols, 128)] = tile
        else:
            lab[pl.ds(TOP, rows), pl.ds(cols, 128)] = tile.astype(jnp.int32)

    groups = rows // 8 + 2

    def right_side(g, _):
        start = pl.multiple_of(g * 8, 8)
        here = lab[pl.ds(start, 8), :]
        total = zero
        for k in range(kinds):
            mid = src[k, pl.ds(start, 8), :]
            term = 4.0 * mid - neighbour_sum(src, (k,), start, mid, width)
            total = jnp.where(here == k, term, total)
        vec[0, pl.ds(start, 8), :] = total
        return 0

    lax.fori_loop(1, groups + 1, right_side, 0)

    def share(g):
        which = jnp.where(g == 1, 0, jnp.where(g == groups, 2, 1))
        return mask[which]

    def apply_to(which):
        def body(g, _):
            start = pl.multiple_of(g * 8, 8)
            mid = vec[which, pl.ds(start, 8), :]
            vec[which + 1, pl.ds(start, 8), :] = share(g) * neighbour_sum(
                vec, (which,), start, mid, width)
            return 0

        lax.fori_loop(1, groups + 1, body, 0)

    for which in range(ITERS - 1):
        apply_to(which)

    def products(g, sums):
        start = pl.multiple_of(g * 8, 8)
        powers = [vec[w, pl.ds(start, 8), :] for w in range(ITERS)]
        powers.append(0.25 * neighbour_sum(vec, (ITERS - 1,), start, powers[-1], width))
        return tuple(
            s + fold_lanes(powers[i // 2] * powers[(i + 1) // 2], cols)
            for i, s in enumerate(sums)
        )

    sums = lax.fori_loop(
        2, groups, products, tuple(jnp.zeros((8, 128), jnp.float32) for _ in range(2 * ITERS)))
    lane1 = lax.broadcasted_iota(jnp.int32, (1, 128), 1)
    mine = jnp.zeros((1, 128), jnp.float32)
    for i, s in enumerate(sums):
        mine = jnp.where(lane1 == i, jnp.sum(s, keepdims=True), mine)
    moment[me] = mine

    def tell(step, _):
        other = lax.rem(me + step, n)
        pltpu.make_async_remote_copy(
            src_ref=moment.at[me], dst_ref=moment.at[me], send_sem=mom_send, recv_sem=mom_recv,
            device_id=(other // n_col, lax.rem(other, n_col)), device_id_type=MESH,
        ).start()
        return 0

    lax.fori_loop(1, n, tell, 0)
    everyone = moment.at[pl.ds(0, n - 1)]
    pltpu.make_async_copy(everyone, everyone, mom_recv).wait()
    total = jnp.sum(moment[...], axis=0)
    moments = [
        jnp.sum(jnp.where(lane1 == i, total, 0.0), axis=1, keepdims=True) for i in range(2 * ITERS)
    ]
    coords = [jnp.broadcast_to(c, (8, cols)) for c in coefficients(moments)]

    def combine(g, _):
        start = pl.multiple_of(g * 8, 8)
        strip = coords[0] * vec[0, pl.ds(start + TOP, 8), pl.ds(0, cols)]
        for w in range(1, ITERS):
            strip = strip + coords[w] * vec[w, pl.ds(start + TOP, 8), pl.ds(0, cols)]
        blend_ref[pl.ds(start, 8), :] = strip
        return 0

    lax.fori_loop(0, rows // 8, combine, 0)

    pool = jnp.where(
        lax.broadcasted_iota(jnp.int32, (256, 128), 0) // 2
        == lax.broadcasted_iota(jnp.int32, (256, 128), 1), 0.25, 0.0).astype(jnp.bfloat16)

    def average(values, slot):
        total = None
        for _ in range(3):
            piece = values.astype(jnp.bfloat16)
            values = values - piece.astype(jnp.float32)
            part = jnp.dot(piece, pool, preferred_element_type=jnp.float32)
            total = part if total is None else total + part
        lines = values.shape[0]
        half[slot, 0:lines, :] = total
        return half[slot, pl.ds(0, lines // 2, stride=2), :] + half[
            slot, pl.ds(1, lines // 2, stride=2), :]

    for tile in range(cols // 256):
        fine_ref[:, tile * 128:(tile + 1) * 128] = average(
            blend_ref[:, tile * 256:(tile + 1) * 256], tile)
    own = pl.ds(pl.multiple_of(row * (rows // 4), 8), rows // 4)
    for tile in range(cols // 512):
        mid_all[own, pl.ds(tile * 128, 128)] = average(
            fine_ref[:, tile * 256:(tile + 1) * 256], tile)

    def spread(step, _):
        other = lax.rem(row + step, n_row)
        pltpu.make_async_remote_copy(
            src_ref=mid_all.at[own], dst_ref=mid_all.at[own], send_sem=mid_send, recv_sem=mid_recv,
            device_id=(other, col), device_id_type=MESH,
        ).start()
        return 0

    lax.fori_loop(1, n_row, spread, 0)
    others = mid_all.at[pl.ds(0, (n_row - 1) * (rows // 4))]
    pltpu.make_async_copy(others, others, mid_recv).wait()
    mid_ref[...] = mid_all[...]
    for tile in range(cols // 1024):
        coarse_ref[:, tile * 128:(tile + 1) * 128] = average(
            mid_all[:, tile * 256:(tile + 1) * 256], tile)

    for there, copy, back in sends:
        pl.when(there)(copy.wait_send)
    pltpu.make_async_copy(everyone, everyone, mom_send).wait()
    pltpu.make_async_copy(others, others, mid_send).wait()


def per_device(n_row, n_col, sources, labels):
    kinds, rows, cols = sources.shape
    n = n_row * n_col
    tall, width = rows + 32, cols + 128
    n_pack = HALO * (kinds + 1)
    f32 = jnp.float32
    vmem = pl.BlockSpec(memory_space=pltpu.VMEM)
    return pl.pallas_call(
        functools.partial(kernel, n_row, n_col, rows, cols, kinds),
        out_shape=(
            jax.ShapeDtypeStruct((rows, cols), f32),
            jax.ShapeDtypeStruct((rows // 2, cols // 2), f32),
            jax.ShapeDtypeStruct((n_row * rows // 4, cols // 4), f32),
            jax.ShapeDtypeStruct((n_row * rows // 8, cols // 8), f32),
        ),
        in_specs=[pl.BlockSpec(memory_space=pl.ANY)] * 2,
        out_specs=(vmem,) * 4,
        scratch_shapes=[
            pltpu.VMEM((kinds, tall, width), f32),
            pltpu.VMEM((tall, width), jnp.int32),
            pltpu.VMEM((ITERS, tall, width), f32),
            pltpu.VMEM((3, 8, width), f32),
            pltpu.VMEM((2, n_pack, cols), f32),
            pltpu.VMEM((2, n_pack, rows), f32),
            pltpu.VMEM((2, n_pack, cols), f32),
            pltpu.VMEM((2, n_pack, rows), f32),
            pltpu.VMEM((2, 2, n_pack, 128), f32),
            pltpu.VMEM((n, 1, 128), f32),
            pltpu.VMEM((n_row * rows // 4, cols // 4), f32),
            pltpu.VMEM((cols // 256, max(rows, n_row * rows // 4), 128), f32),
            pltpu.SemaphoreType.DMA((kinds + 1,)),
            pltpu.SemaphoreType.DMA((8,)),
            pltpu.SemaphoreType.DMA((8,)),
            pltpu.SemaphoreType.DMA,
            pltpu.SemaphoreType.DMA,
            pltpu.SemaphoreType.DMA,
            pltpu.SemaphoreType.DMA,
        ],
        compiler_params=pltpu.CompilerParams(collective_id=0, has_side_effects=True),
    )(sources, labels)


def solution(mesh):
    sizes = dict(mesh.shape)
    return jax.shard_map(
        functools.partial(per_device, sizes["row"], sizes["col"]),
        mesh=mesh,
        in_specs=(P(None, "row", "col"), P("row", "col")),
        out_specs=(P("row", "col"), P("row", "col"), P(None, "col"), P(None, "col")),
        check_vma=False,
    )
```

```python
import functools

import jax
import jax.numpy as jnp
from jax import lax
from jax.experimental import pallas as pl
from jax.experimental.pallas import tpu as pltpu
from jax.sharding import PartitionSpec as P

ITERS = 3
MESH = pl.DeviceIdType.MESH
HALO = 4
TOP = 16
SIDES = ((-1, 0), (1, 0), (0, -1), (0, 1), (-1, -1), (-1, 1), (1, -1), (1, 1))


def neighbour_sum(ref, index, start, mid, width):
    above = ref[index + (pl.ds(pl.multiple_of(start - 8, 8), 8), slice(None))]
    below = ref[index + (pl.ds(pl.multiple_of(start + 8, 8), 8), slice(None))]
    sub = lax.broadcasted_iota(jnp.int32, mid.shape, 0)
    up = pltpu.roll(jnp.where(sub == 7, above, mid), 1, axis=0)
    down = pltpu.roll(jnp.where(sub == 0, below, mid), 7, axis=0)
    left = pltpu.roll(mid, 1, axis=1)
    right = pltpu.roll(mid, width - 1, axis=1)
    return (up + down) + (left + right)


def fold_lanes(strip, cols):
    total = strip[:, 0:128]
    for tile in range(1, cols // 128):
        total = total + strip[:, tile * 128:(tile + 1) * 128]
    return total


def quadratic(left, right, moments, shift):
    total = None
    for i, a in enumerate(left):
        for j, b in enumerate(right):
            term = a * b * moments[i + j + shift]
            total = term if total is None else total + term
    return total


def padded_sum(a, b):
    if len(a) < len(b):
        a, b = b, a
    return [x + b[i] if i < len(b) else x for i, x in enumerate(a)]


def coefficients(moments):
    residual = [jnp.ones_like(moments[0])]
    direction = residual
    solution_coords = [jnp.zeros_like(moments[0])]
    norm_now = moments[0]
    for iteration in range(ITERS):
        applied_dot = 4.0 * (
            quadratic(direction, direction, moments, 0)
            - quadratic(direction, direction, moments, 1)
        )
        step = norm_now / applied_dot
        solution_coords = padded_sum(solution_coords, [step * d for d in direction])
        if iteration + 1 < ITERS:
            moved = [-4.0 * step * d for d in direction]
            residual = padded_sum(residual, moved)
            residual = padded_sum(residual, [jnp.zeros_like(step)] + [-m for m in moved])
            norm_next = quadratic(residual, residual, moments, 0)
            ratio = norm_next / norm_now
            direction = padded_sum(residual, [ratio * d for d in direction])
            norm_now = norm_next
    return solution_coords


def pooled(values, half, slot, pool, stride):
    total = None
    for _ in range(3):
        piece = values.astype(jnp.bfloat16)
        values = values - piece.astype(jnp.float32)
        part = jnp.dot(piece, pool, preferred_element_type=jnp.float32)
        total = part if total is None else total + part
    lines = values.shape[0]
    half[slot, 0:lines, :] = total
    result = half[slot, pl.ds(0, lines // stride, stride=stride), :]
    for line in range(1, stride):
        result = result + half[slot, pl.ds(line, lines // stride, stride=stride), :]
    return result


def pool_matrix(stride):
    shape = (128 * stride, 128)
    source, target = (lax.broadcasted_iota(jnp.int32, shape, d) for d in range(2))
    return jnp.where(source // stride == target, 1.0 / (stride * stride), 0.0).astype(jnp.bfloat16)


def gather_kernel(
    n_row, n_col, rows, cols, kinds,
    src_hbm, lab_hbm, vec, mids, coord_ref,
    src, lab, mask, pack_r, pack_c, got_r, got_c, got_d, moment, half,
    load_sem, send_sem, recv_sem, mom_send, mom_recv, mid_send, mid_recv, fwd_send, fwd_recv,
):
    width = cols + 128
    n = n_row * n_col
    row, col = lax.axis_index("row"), lax.axis_index("col")
    me = row * n_col + col
    loads = [
        pltpu.make_async_copy(
            src_hbm.at[k], src.at[k, pl.ds(TOP, rows), pl.ds(0, cols)], load_sem.at[k]
        )
        for k in range(kinds)
    ]
    loads.append(
        pltpu.make_async_copy(lab_hbm, lab.at[pl.ds(TOP, rows), pl.ds(0, cols)], load_sem.at[kinds])
    )
    for load in loads:
        load.start()

    barrier = pltpu.get_barrier_semaphore()

    columns = [col]
    for _ in range(n_col - 1):
        columns.append(jnp.where(columns[-1] + 1 == n_col, 0, columns[-1] + 1))

    def for_all_others(act):
        for c in columns[1:]:
            act(row, c)

        def body(step, _):
            r = row + step
            r = jnp.where(r >= n_row, r - n_row, r)
            for c in columns:
                act(r, c)
            return 0

        lax.fori_loop(1, n_row, body, 0)

    for_all_others(lambda r, c: pl.semaphore_signal(
        barrier, inc=1, device_id=(r, c), device_id_type=MESH))

    first_row, last_row = row == 0, row == n_row - 1
    first_col, last_col = col == 0, col == n_col - 1
    quarter = jnp.full((8, width), 0.25, jnp.float32)
    lane = lax.broadcasted_iota(jnp.int32, (8, width), 1)
    off = ((lane >= cols) & (lane < cols + 64) & last_col) | ((lane >= cols + 64) & first_col)
    inside = jnp.where(off, 0.0, quarter)
    mask[0] = jnp.where(first_row, 0.0, inside)
    mask[1] = inside
    mask[2] = jnp.where(last_row, 0.0, inside)
    zero = jnp.zeros((8, width), jnp.float32)
    for which in range(3):
        vec[which, 0:8] = zero
        vec[which, rows + 24:rows + 32] = zero

    for load in loads:
        load.wait()

    for k in range(kinds + 1):
        def edge(rng, lanes):
            if k < kinds:
                return src[k, rng, lanes]
            return lab[rng, lanes].astype(jnp.float32)

        at = slice(HALO * k, HALO * (k + 1))
        pack_r[0, at, :] = edge(pl.ds(TOP, HALO), pl.ds(0, cols))
        pack_r[1, at, :] = edge(pl.ds(TOP + rows - HALO, HALO), pl.ds(0, cols))
    n_pack = HALO * (kinds + 1)
    tile_lane = lax.broadcasted_iota(jnp.int32, (rows, 128), 1)
    packed = jnp.zeros((rows, 128), jnp.float32)
    for k in range(kinds + 1):
        for side in range(2):
            lanes = pl.ds(0 if side == 0 else cols - 128, 128)
            if k < kinds:
                tile = src[k, pl.ds(TOP, rows), lanes]
            else:
                tile = lab[pl.ds(TOP, rows), lanes].astype(jnp.float32)
            target = side * n_pack + HALO * k
            origin = 0 if side == 0 else 128 - HALO
            if (target - origin) % 128:
                tile = pltpu.roll(tile, (target - origin) % 128, axis=1)
            packed = jnp.where((tile_lane >= target) & (tile_lane < target + HALO), tile, packed)
    turned = jnp.transpose(packed)
    pack_c[0] = turned[0:n_pack]
    pack_c[1] = turned[n_pack:2 * n_pack]

    pl.semaphore_wait(barrier, n - 1)

    sends = []
    for i, (dr, dc) in enumerate(SIDES):
        if dc == 0:
            source = pack_r.at[0 if dr < 0 else 1]
            target = got_r.at[1 if dr < 0 else 0]
        elif dr == 0:
            source = pack_c.at[0 if dc < 0 else 1]
            target = got_c.at[1 if dc < 0 else 0]
        else:
            lanes = pl.ds(0 if dc < 0 else cols - 128, 128)
            source = pack_r.at[0 if dr < 0 else 1, :, lanes]
            target = got_d.at[1 if dr < 0 else 0, 1 if dc < 0 else 0]
        there = jnp.logical_and(
            jnp.logical_and(row + dr >= 0, row + dr < n_row),
            jnp.logical_and(col + dc >= 0, col + dc < n_col),
        )
        opposite = SIDES.index((-dr, -dc))
        device = (
            jnp.clip(row + dr, 0, n_row - 1),
            jnp.clip(col + dc, 0, n_col - 1),
        )
        copy = pltpu.make_async_remote_copy(
            src_ref=source, dst_ref=target, send_sem=send_sem.at[i],
            recv_sem=recv_sem.at[opposite], device_id=device, device_id_type=MESH,
        )
        back = pltpu.make_async_remote_copy(
            src_ref=source, dst_ref=got_r.at[0 if dr < 0 else 1] if dc == 0 else (
                got_c.at[0 if dc < 0 else 1] if dr == 0
                else got_d.at[0 if dr < 0 else 1, 0 if dc < 0 else 1]),
            send_sem=send_sem.at[i], recv_sem=recv_sem.at[i],
            device_id=device, device_id_type=MESH,
        )
        sends.append((there, copy, back))
        pl.when(there)(copy.start)
    for there, copy, back in sends:
        pl.when(there)(back.wait_recv)

    halo_lane = lax.broadcasted_iota(jnp.int32, (HALO, 128), 1)
    for side in range(2):
        missing_row = first_row if side == 0 else last_row
        base = TOP - HALO if side == 0 else TOP + rows
        other = TOP - 8 if side == 0 else TOP + rows + HALO
        for k in range(kinds + 1):
            fill = jnp.float32(0.0 if k < kinds else -1.0)
            at = slice(HALO * k, HALO * (k + 1))
            wide = jnp.where(missing_row, fill, got_r[side, at, :])
            right = jnp.where(
                (halo_lane < HALO) & jnp.logical_not(missing_row | last_col),
                got_d[side, 1, at, :], fill)
            corner = jnp.where(
                (halo_lane >= 128 - HALO) & jnp.logical_not(missing_row | first_col),
                got_d[side, 0, at, :], right)
            empty = jnp.full((HALO, width), fill)
            if k < kinds:
                src[k, pl.ds(base, HALO), pl.ds(0, cols)] = wide
                src[k, pl.ds(base, HALO), pl.ds(cols, 128)] = corner
                src[k, pl.ds(other, HALO), :] = empty
            else:
                lab[pl.ds(base, HALO), pl.ds(0, cols)] = wide.astype(jnp.int32)
                lab[pl.ds(base, HALO), pl.ds(cols, 128)] = corner.astype(jnp.int32)
                lab[pl.ds(other, HALO), :] = empty.astype(jnp.int32)
    both = jnp.concatenate(
        [
            got_c[1],
            got_c[0],
            jnp.zeros((128 - 2 * n_pack, rows), jnp.float32),
        ],
        axis=0,
    )
    unturned = jnp.transpose(both)
    for k in range(kinds + 1):
        fill = jnp.float32(0.0 if k < kinds else -1.0)
        right = pltpu.roll(unturned, (-HALO * k) % 128, axis=1)
        left = pltpu.roll(unturned, (128 - HALO - n_pack - HALO * k) % 128, axis=1)
        tile = jnp.where((tile_lane < HALO) & jnp.logical_not(last_col), right, fill)
        tile = jnp.where((tile_lane >= 128 - HALO) & jnp.logical_not(first_col), left, tile)
        if k < kinds:
            src[k, pl.ds(TOP, rows), pl.ds(cols, 128)] = tile
        else:
            lab[pl.ds(TOP, rows), pl.ds(cols, 128)] = tile.astype(jnp.int32)

    groups = rows // 8 + 2

    def right_side(g, _):
        start = pl.multiple_of(g * 8, 8)
        here = lab[pl.ds(start, 8), :]
        total = zero
        for k in range(kinds):
            mid = src[k, pl.ds(start, 8), :]
            term = 4.0 * mid - neighbour_sum(src, (k,), start, mid, width)
            total = jnp.where(here == k, term, total)
        vec[0, pl.ds(start, 8), :] = total
        return 0

    lax.fori_loop(1, groups + 1, right_side, 0, unroll=2)

    def share(g):
        which = jnp.where(g == 1, 0, jnp.where(g == groups, 2, 1))
        return mask[which]

    def apply_to(which):
        def body(g, _):
            start = pl.multiple_of(g * 8, 8)
            mid = vec[which, pl.ds(start, 8), :]
            vec[which + 1, pl.ds(start, 8), :] = share(g) * neighbour_sum(
                vec, (which,), start, mid, width)
            return 0

        lax.fori_loop(1, groups + 1, body, 0, unroll=3)

    chips = n_row // 2
    partner = row + 1 - 2 * lax.rem(row, 2)
    quad = rows // 4
    pool = pool_matrix(4)

    def block(w, owner):
        return mids.at[w, pl.ds(pl.multiple_of(owner * quad, 8), quad)]

    def peer(step):
        other = row + 2 * step
        return jnp.where(other >= n_row, other - n_row, other)

    def hand(w, owner, target, send, recv):
        return pltpu.make_async_remote_copy(
            src_ref=block(w, owner), dst_ref=block(w, owner), send_sem=send, recv_sem=recv,
            device_id=(target, col), device_id_type=MESH)

    def gather(w):
        for tile in range(cols // 512):
            mids[w, pl.ds(pl.multiple_of(row * quad, 8), quad), pl.ds(tile * 128, 128)] = pooled(
                vec[w, pl.ds(TOP, rows), pl.ds(tile * 512, 512)], half,
                w * (cols // 512) + tile, pool, 4)
        hops = [
            hand(w, row, peer(step), mid_send.at[w, step], mid_recv.at[w, step])
            for step in range(1, chips)
        ]
        hops.append(hand(w, row, partner, mid_send.at[w, 0], mid_recv.at[w, 0]))
        for hop in hops:
            hop.start()
        return hops

    hops = []
    for which in range(ITERS - 1):
        hops += gather(which)
        apply_to(which)
    hops += gather(ITERS - 1)

    def products(g, sums):
        start = pl.multiple_of(g * 8, 8)
        powers = [vec[w, pl.ds(start, 8), :] for w in range(ITERS)]
        powers.append(0.25 * neighbour_sum(vec, (ITERS - 1,), start, powers[-1], width))
        return tuple(
            s + fold_lanes(powers[i // 2] * powers[(i + 1) // 2], cols)
            for i, s in enumerate(sums)
        )

    sums = lax.fori_loop(
        2, groups, products, tuple(jnp.zeros((8, 128), jnp.float32) for _ in range(2 * ITERS)), unroll=2)
    lane1 = lax.broadcasted_iota(jnp.int32, (1, 128), 1)
    mine = jnp.zeros((1, 128), jnp.float32)
    for i, s in enumerate(sums):
        mine = jnp.where(lane1 == i, jnp.sum(s, keepdims=True), mine)
    moment[me] = mine

    for_all_others(lambda r, c: pltpu.make_async_remote_copy(
        src_ref=moment.at[me], dst_ref=moment.at[me], send_sem=mom_send, recv_sem=mom_recv,
        device_id=(r, c), device_id_type=MESH).start())
    everyone = moment.at[pl.ds(0, n - 1)]
    pltpu.make_async_copy(everyone, everyone, mom_recv).wait()
    total = jnp.sum(moment[...], axis=0)
    moments = [
        jnp.sum(jnp.where(lane1 == i, total, 0.0), axis=1, keepdims=True) for i in range(2 * ITERS)
    ]
    for w, c in enumerate(coefficients(moments)):
        coord_ref[w] = jnp.broadcast_to(c, (8, 128))

    def source_of(step):
        other = row - 2 * step
        return jnp.where(other < 0, other + n_row, other)

    def other_core(owner):
        return owner + 1 - 2 * lax.rem(owner, 2)

    forwards = []
    for w in range(ITERS):
        for step in range(1, chips):
            owner = source_of(step)
            hand(w, owner, partner, mid_send.at[w, step], mid_recv.at[w, step]).wait_recv()
            forward = hand(w, owner, partner, fwd_send.at[w, step], fwd_recv.at[w, step])
            forward.start()
            forwards.append(forward)
    for w in range(ITERS):
        hand(w, partner, partner, mid_send.at[w, 0], mid_recv.at[w, 0]).wait_recv()
        for step in range(1, chips):
            hand(w, other_core(source_of(step)), partner,
                 fwd_send.at[w, step], fwd_recv.at[w, step]).wait_recv()
    for hop in hops:
        hop.wait_send()
    for forward in forwards:
        forward.wait_send()
    for there, copy, back in sends:
        pl.when(there)(copy.wait_send)
    pltpu.make_async_copy(everyone, everyone, mom_send).wait()


def finish_kernel(
    rows, cols, vec, mids, coord_ref, blend_out, fine_out, mid_out, coarse_out,
    blend, fine, mid, coarse, half, out_sem,
):
    pool = pool_matrix(2)

    def leave(slot, source, target):
        copy = pltpu.make_async_copy(source, target, out_sem.at[slot])
        copy.start()
        return copy

    def combine(source, target, lines, lanes, first):
        coords = [jnp.concatenate([coord_ref[w]] * (lanes // 128), axis=1) for w in range(ITERS)]

        def body(g, _):
            start = pl.multiple_of(g * 8, 8)
            strip = None
            for w in range(ITERS):
                term = coords[w] * source[w, pl.ds(start + first, 8), pl.ds(0, lanes)]
                strip = term if strip is None else strip + term
            target[pl.ds(start, 8), :] = strip
            return 0

        lax.fori_loop(0, lines // 8, body, 0, unroll=4)

    combine(vec, blend, rows, cols, TOP)
    copies = [leave(0, blend, blend_out)]
    tall, wide = mid.shape
    combine(mids, mid, tall, wide, 0)
    copies.append(leave(1, mid, mid_out))
    for tile in range(cols // 256):
        fine[:, tile * 128:(tile + 1) * 128] = pooled(
            blend[:, tile * 256:(tile + 1) * 256], half, tile, pool, 2)
    copies.append(leave(2, fine, fine_out))
    for tile in range(wide // 256):
        coarse[:, tile * 128:(tile + 1) * 128] = pooled(
            mid[:, tile * 256:(tile + 1) * 256], half, cols // 256 + tile, pool, 2)
    copies.append(leave(3, coarse, coarse_out))
    for copy in copies:
        copy.wait()


def per_device(n_row, n_col, sources, labels):
    kinds, rows, cols = sources.shape
    n = n_row * n_col
    tall, width = rows + 32, cols + 128
    n_pack = HALO * (kinds + 1)
    f32 = jnp.float32
    vmem = pl.BlockSpec(memory_space=pltpu.VMEM)
    hbm = pl.BlockSpec(memory_space=pltpu.HBM)
    mid_shape = (n_row * rows // 4, cols // 4)
    coarse_shape = (n_row * rows // 8, cols // 8)
    chips = n_row // 2
    dma = pltpu.SemaphoreType.DMA
    vec, mids, coords = pl.pallas_call(
        functools.partial(gather_kernel, n_row, n_col, rows, cols, kinds),
        out_shape=(
            jax.ShapeDtypeStruct((ITERS, tall, width), f32),
            jax.ShapeDtypeStruct((ITERS,) + mid_shape, f32),
            jax.ShapeDtypeStruct((ITERS, 8, 128), f32),
        ),
        in_specs=[hbm] * 2,
        out_specs=(vmem,) * 3,
        scratch_shapes=[
            pltpu.VMEM((kinds, tall, width), f32),
            pltpu.VMEM((tall, width), jnp.int32),
            pltpu.VMEM((3, 8, width), f32),
            pltpu.VMEM((2, n_pack, cols), f32),
            pltpu.VMEM((2, n_pack, rows), f32),
            pltpu.VMEM((2, n_pack, cols), f32),
            pltpu.VMEM((2, n_pack, rows), f32),
            pltpu.VMEM((2, 2, n_pack, 128), f32),
            pltpu.VMEM((n, 1, 128), f32),
            pltpu.VMEM((ITERS * (cols // 512), rows, 128), f32),
            dma((kinds + 1,)),
            dma((8,)),
            dma((8,)),
            dma,
            dma,
            dma((ITERS, chips)),
            dma((ITERS, chips)),
            dma((ITERS, chips)),
            dma((ITERS, chips)),
        ],
        compiler_params=pltpu.CompilerParams(
            collective_id=0, has_side_effects=True, vmem_limit_bytes=20 * 2**20),
    )(
        pltpu.with_memory_space_constraint(sources, pltpu.HBM),
        pltpu.with_memory_space_constraint(labels, pltpu.HBM),
    )
    return pl.pallas_call(
        functools.partial(finish_kernel, rows, cols),
        out_shape=(
            jax.ShapeDtypeStruct((rows, cols), f32),
            jax.ShapeDtypeStruct((rows // 2, cols // 2), f32),
            jax.ShapeDtypeStruct(mid_shape, f32),
            jax.ShapeDtypeStruct(coarse_shape, f32),
        ),
        in_specs=[vmem] * 3,
        out_specs=(hbm,) * 4,
        scratch_shapes=[
            pltpu.VMEM((rows, cols), f32),
            pltpu.VMEM((rows // 2, cols // 2), f32),
            pltpu.VMEM(mid_shape, f32),
            pltpu.VMEM(coarse_shape, f32),
            pltpu.VMEM((cols // 256 + cols // 1024, max(rows, mid_shape[0]), 128), f32),
            dma((4,)),
        ],
        compiler_params=pltpu.CompilerParams(vmem_limit_bytes=20 * 2**20),
    )(vec, mids, coords)


def solution(mesh):
    sizes = dict(mesh.shape)
    return jax.shard_map(
        functools.partial(per_device, sizes["row"], sizes["col"]),
        mesh=mesh,
        in_specs=(P(None, "row", "col"), P("row", "col")),
        out_specs=(P("row", "col"), P("row", "col"), P(None, "col"), P(None, "col")),
        check_vma=False,
    )
```

```python
import functools

import jax
import jax.numpy as jnp
from jax import lax
from jax.experimental import pallas as pl
from jax.experimental.pallas import tpu as pltpu
from jax.sharding import PartitionSpec as P

ITERS = 3
MESH = pl.DeviceIdType.MESH
HALO = 4
TOP = 16
SIDES = ((-1, 0), (1, 0), (0, -1), (0, 1), (-1, -1), (-1, 1), (1, -1), (1, 1))


def neighbour_sum(ref, index, start, mid, width):
    above = ref[index + (pl.ds(pl.multiple_of(start - 8, 8), 8), slice(None))]
    below = ref[index + (pl.ds(pl.multiple_of(start + 8, 8), 8), slice(None))]
    sub = lax.broadcasted_iota(jnp.int32, mid.shape, 0)
    up = pltpu.roll(jnp.where(sub == 7, above, mid), 1, axis=0)
    down = pltpu.roll(jnp.where(sub == 0, below, mid), 7, axis=0)
    left = pltpu.roll(mid, 1, axis=1)
    right = pltpu.roll(mid, width - 1, axis=1)
    return (up + down) + (left + right)


def fold_lanes(strip, cols):
    total = strip[:, 0:128]
    for tile in range(1, cols // 128):
        total = total + strip[:, tile * 128:(tile + 1) * 128]
    return total


def quadratic(left, right, moments, shift):
    total = None
    for i, a in enumerate(left):
        for j, b in enumerate(right):
            term = a * b * moments[i + j + shift]
            total = term if total is None else total + term
    return total


def padded_sum(a, b):
    if len(a) < len(b):
        a, b = b, a
    return [x + b[i] if i < len(b) else x for i, x in enumerate(a)]


def coefficients(moments):
    residual = [jnp.ones_like(moments[0])]
    direction = residual
    solution_coords = [jnp.zeros_like(moments[0])]
    norm_now = moments[0]
    for iteration in range(ITERS):
        applied_dot = 4.0 * (
            quadratic(direction, direction, moments, 0)
            - quadratic(direction, direction, moments, 1)
        )
        step = norm_now / applied_dot
        solution_coords = padded_sum(solution_coords, [step * d for d in direction])
        if iteration + 1 < ITERS:
            moved = [-4.0 * step * d for d in direction]
            residual = padded_sum(residual, moved)
            residual = padded_sum(residual, [jnp.zeros_like(step)] + [-m for m in moved])
            norm_next = quadratic(residual, residual, moments, 0)
            ratio = norm_next / norm_now
            direction = padded_sum(residual, [ratio * d for d in direction])
            norm_now = norm_next
    return solution_coords


def pooled(values, half, slot, pool, stride):
    total = None
    for _ in range(3):
        piece = values.astype(jnp.bfloat16)
        values = values - piece.astype(jnp.float32)
        part = jnp.dot(piece, pool, preferred_element_type=jnp.float32)
        total = part if total is None else total + part
    lines = values.shape[0]
    half[slot, 0:lines, :] = total
    result = half[slot, pl.ds(0, lines // stride, stride=stride), :]
    for line in range(1, stride):
        result = result + half[slot, pl.ds(line, lines // stride, stride=stride), :]
    return result


def pool_matrix(stride):
    shape = (128 * stride, 128)
    source, target = (lax.broadcasted_iota(jnp.int32, shape, d) for d in range(2))
    return jnp.where(source // stride == target, 1.0 / (stride * stride), 0.0).astype(jnp.bfloat16)


def gather_kernel(
    n_row, n_col, rows, cols, kinds,
    src_hbm, lab_hbm, vec, mids, coord_ref,
    src, lab, mask, pack_r, pack_c, got_r, got_c, got_d, mom_col, mom_row, half,
    load_sem, send_sem, recv_sem, mom_send, mom_recv, mid_send, mid_recv, fwd_send, fwd_recv,
):
    width = cols + 128
    row, col = lax.axis_index("row"), lax.axis_index("col")
    loads = [
        pltpu.make_async_copy(
            src_hbm.at[k], src.at[k, pl.ds(TOP, rows), pl.ds(0, cols)], load_sem.at[k]
        )
        for k in range(kinds)
    ]
    loads.append(
        pltpu.make_async_copy(lab_hbm, lab.at[pl.ds(TOP, rows), pl.ds(0, cols)], load_sem.at[kinds])
    )
    for load in loads:
        load.start()

    barrier = pltpu.get_barrier_semaphore()

    def ring(place, count):
        places = []
        for _ in range(count - 1):
            place = jnp.where(place + 1 == count, 0, place + 1)
            places.append(place)
        return places

    col_peers = [(row, c) for c in ring(col, n_col)]
    row_peers = [(r, col) for r in ring(row, n_row)]

    def greet(device):
        pl.semaphore_signal(barrier, inc=1, device_id=device, device_id_type=MESH)

    for dr in (-1, 1):
        for dc in (-1, 1):
            there = jnp.logical_and(
                jnp.logical_and(row + dr >= 0, row + dr < n_row),
                jnp.logical_and(col + dc >= 0, col + dc < n_col),
            )
            device = (jnp.clip(row + dr, 0, n_row - 1), jnp.clip(col + dc, 0, n_col - 1))
            pl.when(there)(functools.partial(greet, device))
    for device in col_peers + row_peers:
        greet(device)
    corners = (
        jnp.where(row == 0, 0, 1) + jnp.where(row == n_row - 1, 0, 1)
    ) * (jnp.where(col == 0, 0, 1) + jnp.where(col == n_col - 1, 0, 1))

    first_row, last_row = row == 0, row == n_row - 1
    first_col, last_col = col == 0, col == n_col - 1
    quarter = jnp.full((8, width), 0.25, jnp.float32)
    lane = lax.broadcasted_iota(jnp.int32, (8, width), 1)
    off = ((lane >= cols) & (lane < cols + 64) & last_col) | ((lane >= cols + 64) & first_col)
    inside = jnp.where(off, 0.0, quarter)
    mask[0] = jnp.where(first_row, 0.0, inside)
    mask[1] = inside
    mask[2] = jnp.where(last_row, 0.0, inside)
    zero = jnp.zeros((8, width), jnp.float32)
    for which in range(3):
        vec[which, 0:8] = zero
        vec[which, rows + 24:rows + 32] = zero

    for load in loads:
        load.wait()

    for k in range(kinds + 1):
        def edge(rng, lanes):
            if k < kinds:
                return src[k, rng, lanes]
            return lab[rng, lanes].astype(jnp.float32)

        at = slice(HALO * k, HALO * (k + 1))
        pack_r[0, at, :] = edge(pl.ds(TOP, HALO), pl.ds(0, cols))
        pack_r[1, at, :] = edge(pl.ds(TOP + rows - HALO, HALO), pl.ds(0, cols))
    n_pack = HALO * (kinds + 1)
    tile_lane = lax.broadcasted_iota(jnp.int32, (rows, 128), 1)
    packed = jnp.zeros((rows, 128), jnp.float32)
    for k in range(kinds + 1):
        for side in range(2):
            lanes = pl.ds(0 if side == 0 else cols - 128, 128)
            if k < kinds:
                tile = src[k, pl.ds(TOP, rows), lanes]
            else:
                tile = lab[pl.ds(TOP, rows), lanes].astype(jnp.float32)
            target = side * n_pack + HALO * k
            origin = 0 if side == 0 else 128 - HALO
            if (target - origin) % 128:
                tile = pltpu.roll(tile, (target - origin) % 128, axis=1)
            packed = jnp.where((tile_lane >= target) & (tile_lane < target + HALO), tile, packed)
    turned = jnp.transpose(packed)
    pack_c[0] = turned[0:n_pack]
    pack_c[1] = turned[n_pack:2 * n_pack]

    pl.semaphore_wait(barrier, n_row + n_col - 2 + corners)

    sends = []
    for i, (dr, dc) in enumerate(SIDES):
        if dc == 0:
            source = pack_r.at[0 if dr < 0 else 1]
            target = got_r.at[1 if dr < 0 else 0]
        elif dr == 0:
            source = pack_c.at[0 if dc < 0 else 1]
            target = got_c.at[1 if dc < 0 else 0]
        else:
            lanes = pl.ds(0 if dc < 0 else cols - 128, 128)
            source = pack_r.at[0 if dr < 0 else 1, :, lanes]
            target = got_d.at[1 if dr < 0 else 0, 1 if dc < 0 else 0]
        there = jnp.logical_and(
            jnp.logical_and(row + dr >= 0, row + dr < n_row),
            jnp.logical_and(col + dc >= 0, col + dc < n_col),
        )
        opposite = SIDES.index((-dr, -dc))
        device = (
            jnp.clip(row + dr, 0, n_row - 1),
            jnp.clip(col + dc, 0, n_col - 1),
        )
        copy = pltpu.make_async_remote_copy(
            src_ref=source, dst_ref=target, send_sem=send_sem.at[i],
            recv_sem=recv_sem.at[opposite], device_id=device, device_id_type=MESH,
        )
        back = pltpu.make_async_remote_copy(
            src_ref=source, dst_ref=got_r.at[0 if dr < 0 else 1] if dc == 0 else (
                got_c.at[0 if dc < 0 else 1] if dr == 0
                else got_d.at[0 if dr < 0 else 1, 0 if dc < 0 else 1]),
            send_sem=send_sem.at[i], recv_sem=recv_sem.at[i],
            device_id=device, device_id_type=MESH,
        )
        sends.append((there, copy, back))
        pl.when(there)(copy.start)
    for there, copy, back in sends:
        pl.when(there)(back.wait_recv)

    halo_lane = lax.broadcasted_iota(jnp.int32, (HALO, 128), 1)
    for side in range(2):
        missing_row = first_row if side == 0 else last_row
        base = TOP - HALO if side == 0 else TOP + rows
        other = TOP - 8 if side == 0 else TOP + rows + HALO
        for k in range(kinds + 1):
            fill = jnp.float32(0.0 if k < kinds else -1.0)
            at = slice(HALO * k, HALO * (k + 1))
            wide = jnp.where(missing_row, fill, got_r[side, at, :])
            right = jnp.where(
                (halo_lane < HALO) & jnp.logical_not(missing_row | last_col),
                got_d[side, 1, at, :], fill)
            corner = jnp.where(
                (halo_lane >= 128 - HALO) & jnp.logical_not(missing_row | first_col),
                got_d[side, 0, at, :], right)
            empty = jnp.full((HALO, width), fill)
            if k < kinds:
                src[k, pl.ds(base, HALO), pl.ds(0, cols)] = wide
                src[k, pl.ds(base, HALO), pl.ds(cols, 128)] = corner
                src[k, pl.ds(other, HALO), :] = empty
            else:
                lab[pl.ds(base, HALO), pl.ds(0, cols)] = wide.astype(jnp.int32)
                lab[pl.ds(base, HALO), pl.ds(cols, 128)] = corner.astype(jnp.int32)
                lab[pl.ds(other, HALO), :] = empty.astype(jnp.int32)
    both = jnp.concatenate(
        [
            got_c[1],
            got_c[0],
            jnp.zeros((128 - 2 * n_pack, rows), jnp.float32),
        ],
        axis=0,
    )
    unturned = jnp.transpose(both)
    for k in range(kinds + 1):
        fill = jnp.float32(0.0 if k < kinds else -1.0)
        right = pltpu.roll(unturned, (-HALO * k) % 128, axis=1)
        left = pltpu.roll(unturned, (128 - HALO - n_pack - HALO * k) % 128, axis=1)
        tile = jnp.where((tile_lane < HALO) & jnp.logical_not(last_col), right, fill)
        tile = jnp.where((tile_lane >= 128 - HALO) & jnp.logical_not(first_col), left, tile)
        if k < kinds:
            src[k, pl.ds(TOP, rows), pl.ds(cols, 128)] = tile
        else:
            lab[pl.ds(TOP, rows), pl.ds(cols, 128)] = tile.astype(jnp.int32)

    groups = rows // 8 + 2

    def right_side(g, _):
        start = pl.multiple_of(g * 8, 8)
        here = lab[pl.ds(start, 8), :]
        total = zero
        for k in range(kinds):
            mid = src[k, pl.ds(start, 8), :]
            term = 4.0 * mid - neighbour_sum(src, (k,), start, mid, width)
            total = jnp.where(here == k, term, total)
        vec[0, pl.ds(start, 8), :] = total
        return 0

    lax.fori_loop(1, groups + 1, right_side, 0, unroll=2)

    def share(g):
        which = jnp.where(g == 1, 0, jnp.where(g == groups, 2, 1))
        return mask[which]

    def apply_to(which):
        def body(g, _):
            start = pl.multiple_of(g * 8, 8)
            mid = vec[which, pl.ds(start, 8), :]
            vec[which + 1, pl.ds(start, 8), :] = share(g) * neighbour_sum(
                vec, (which,), start, mid, width)
            return 0

        lax.fori_loop(1, groups + 1, body, 0, unroll=3)

    chips = n_row // 2
    partner = row + 1 - 2 * lax.rem(row, 2)
    quad = rows // 4
    pool = pool_matrix(4)

    def block(w, owner):
        return mids.at[w, pl.ds(pl.multiple_of(owner * quad, 8), quad)]

    def peer(step):
        other = row + 2 * step
        return jnp.where(other >= n_row, other - n_row, other)

    def hand(w, owner, target, send, recv):
        return pltpu.make_async_remote_copy(
            src_ref=block(w, owner), dst_ref=block(w, owner), send_sem=send, recv_sem=recv,
            device_id=(target, col), device_id_type=MESH)

    def gather(w):
        for tile in range(cols // 512):
            mids[w, pl.ds(pl.multiple_of(row * quad, 8), quad), pl.ds(tile * 128, 128)] = pooled(
                vec[w, pl.ds(TOP, rows), pl.ds(tile * 512, 512)], half,
                w * (cols // 512) + tile, pool, 4)
        hops = [
            hand(w, row, peer(step), mid_send.at[w, step], mid_recv.at[w, step])
            for step in range(1, chips)
        ]
        hops.append(hand(w, row, partner, mid_send.at[w, 0], mid_recv.at[w, 0]))
        for hop in hops:
            hop.start()
        return hops

    hops = []
    for which in range(ITERS - 1):
        hops += gather(which)
        apply_to(which)

    def products(g, sums):
        start = pl.multiple_of(g * 8, 8)
        powers = [vec[w, pl.ds(start, 8), :] for w in range(ITERS)]
        powers.append(0.25 * neighbour_sum(vec, (ITERS - 1,), start, powers[-1], width))
        return tuple(
            s + fold_lanes(powers[i // 2] * powers[(i + 1) // 2], cols)
            for i, s in enumerate(sums)
        )

    sums = lax.fori_loop(
        2, groups, products, tuple(jnp.zeros((8, 128), jnp.float32) for _ in range(2 * ITERS)), unroll=2)
    lane1 = lax.broadcasted_iota(jnp.int32, (1, 128), 1)
    mine = jnp.zeros((1, 128), jnp.float32)
    for i, s in enumerate(sums):
        mine = jnp.where(lane1 == i, jnp.sum(s, keepdims=True), mine)

    def share_out(buffer, slot, value, peers, send, recv):
        buffer[slot] = value
        for device in peers:
            pltpu.make_async_remote_copy(
                src_ref=buffer.at[slot], dst_ref=buffer.at[slot], send_sem=send, recv_sem=recv,
                device_id=device, device_id_type=MESH).start()
        return buffer.at[pl.ds(0, len(peers))]

    col_rest = share_out(mom_col, col, mine, col_peers, mom_send.at[0], mom_recv.at[0])
    hops += gather(ITERS - 1)
    pltpu.make_async_copy(col_rest, col_rest, mom_recv.at[0]).wait()
    part = jnp.sum(mom_col[...], axis=0)
    row_rest = share_out(mom_row, row, part, row_peers, mom_send.at[1], mom_recv.at[1])

    def source_of(step):
        other = row - 2 * step
        return jnp.where(other < 0, other + n_row, other)

    def other_core(owner):
        return owner + 1 - 2 * lax.rem(owner, 2)

    forwards = []
    for w in range(ITERS):
        for step in range(1, chips):
            owner = source_of(step)
            hand(w, owner, partner, mid_send.at[w, step], mid_recv.at[w, step]).wait_recv()
            forward = hand(w, owner, partner, fwd_send.at[w, step], fwd_recv.at[w, step])
            forward.start()
            forwards.append(forward)
    for w in range(ITERS):
        hand(w, partner, partner, mid_send.at[w, 0], mid_recv.at[w, 0]).wait_recv()
        for step in range(1, chips):
            hand(w, other_core(source_of(step)), partner,
                 fwd_send.at[w, step], fwd_recv.at[w, step]).wait_recv()
    pltpu.make_async_copy(row_rest, row_rest, mom_recv.at[1]).wait()
    total = jnp.sum(mom_row[...], axis=0)
    moments = [
        jnp.sum(jnp.where(lane1 == i, total, 0.0), axis=1, keepdims=True) for i in range(2 * ITERS)
    ]
    for w, c in enumerate(coefficients(moments)):
        coord_ref[w] = jnp.broadcast_to(c, (8, 128))
    for hop in hops:
        hop.wait_send()
    for forward in forwards:
        forward.wait_send()
    for there, copy, back in sends:
        pl.when(there)(copy.wait_send)
    pltpu.make_async_copy(col_rest, col_rest, mom_send.at[0]).wait()
    pltpu.make_async_copy(row_rest, row_rest, mom_send.at[1]).wait()


def finish_kernel(
    rows, cols, vec, mids, coord_ref, blend_out, fine_out, mid_out, coarse_out,
    blend, fine, mid, coarse, half, out_sem,
):
    pool = pool_matrix(2)

    def leave(slot, source, target):
        copy = pltpu.make_async_copy(source, target, out_sem.at[slot])
        copy.start()
        return copy

    def combine(source, target, lines, lanes, first):
        coords = [jnp.concatenate([coord_ref[w]] * (lanes // 128), axis=1) for w in range(ITERS)]

        def body(g, _):
            start = pl.multiple_of(g * 8, 8)
            strip = None
            for w in range(ITERS):
                term = coords[w] * source[w, pl.ds(start + first, 8), pl.ds(0, lanes)]
                strip = term if strip is None else strip + term
            target[pl.ds(start, 8), :] = strip
            return 0

        lax.fori_loop(0, lines // 8, body, 0, unroll=4)

    combine(vec, blend, rows, cols, TOP)
    copies = [leave(0, blend, blend_out)]
    tall, wide = mid.shape
    combine(mids, mid, tall, wide, 0)
    copies.append(leave(1, mid, mid_out))
    for tile in range(cols // 256):
        fine[:, tile * 128:(tile + 1) * 128] = pooled(
            blend[:, tile * 256:(tile + 1) * 256], half, tile, pool, 2)
    copies.append(leave(2, fine, fine_out))
    for tile in range(wide // 256):
        coarse[:, tile * 128:(tile + 1) * 128] = pooled(
            mid[:, tile * 256:(tile + 1) * 256], half, cols // 256 + tile, pool, 2)
    copies.append(leave(3, coarse, coarse_out))
    for copy in copies:
        copy.wait()


def per_device(n_row, n_col, sources, labels):
    kinds, rows, cols = sources.shape
    tall, width = rows + 32, cols + 128
    n_pack = HALO * (kinds + 1)
    f32 = jnp.float32
    vmem = pl.BlockSpec(memory_space=pltpu.VMEM)
    hbm = pl.BlockSpec(memory_space=pltpu.HBM)
    mid_shape = (n_row * rows // 4, cols // 4)
    coarse_shape = (n_row * rows // 8, cols // 8)
    chips = n_row // 2
    dma = pltpu.SemaphoreType.DMA
    vec, mids, coords = pl.pallas_call(
        functools.partial(gather_kernel, n_row, n_col, rows, cols, kinds),
        out_shape=(
            jax.ShapeDtypeStruct((ITERS, tall, width), f32),
            jax.ShapeDtypeStruct((ITERS,) + mid_shape, f32),
            jax.ShapeDtypeStruct((ITERS, 8, 128), f32),
        ),
        in_specs=[hbm] * 2,
        out_specs=(vmem,) * 3,
        scratch_shapes=[
            pltpu.VMEM((kinds, tall, width), f32),
            pltpu.VMEM((tall, width), jnp.int32),
            pltpu.VMEM((3, 8, width), f32),
            pltpu.VMEM((2, n_pack, cols), f32),
            pltpu.VMEM((2, n_pack, rows), f32),
            pltpu.VMEM((2, n_pack, cols), f32),
            pltpu.VMEM((2, n_pack, rows), f32),
            pltpu.VMEM((2, 2, n_pack, 128), f32),
            pltpu.VMEM((n_col, 1, 128), f32),
            pltpu.VMEM((n_row, 1, 128), f32),
            pltpu.VMEM((ITERS * (cols // 512), rows, 128), f32),
            dma((kinds + 1,)),
            dma((8,)),
            dma((8,)),
            dma((2,)),
            dma((2,)),
            dma((ITERS, chips)),
            dma((ITERS, chips)),
            dma((ITERS, chips)),
            dma((ITERS, chips)),
        ],
        compiler_params=pltpu.CompilerParams(
            collective_id=0, has_side_effects=True, vmem_limit_bytes=20 * 2**20),
    )(
        pltpu.with_memory_space_constraint(sources, pltpu.HBM),
        pltpu.with_memory_space_constraint(labels, pltpu.HBM),
    )
    return pl.pallas_call(
        functools.partial(finish_kernel, rows, cols),
        out_shape=(
            jax.ShapeDtypeStruct((rows, cols), f32),
            jax.ShapeDtypeStruct((rows // 2, cols // 2), f32),
            jax.ShapeDtypeStruct(mid_shape, f32),
            jax.ShapeDtypeStruct(coarse_shape, f32),
        ),
        in_specs=[vmem] * 3,
        out_specs=(hbm,) * 4,
        scratch_shapes=[
            pltpu.VMEM((rows, cols), f32),
            pltpu.VMEM((rows // 2, cols // 2), f32),
            pltpu.VMEM(mid_shape, f32),
            pltpu.VMEM(coarse_shape, f32),
            pltpu.VMEM((cols // 256 + cols // 1024, max(rows, mid_shape[0]), 128), f32),
            dma((4,)),
        ],
        compiler_params=pltpu.CompilerParams(vmem_limit_bytes=20 * 2**20),
    )(vec, mids, coords)


def solution(mesh):
    sizes = dict(mesh.shape)
    return jax.shard_map(
        functools.partial(per_device, sizes["row"], sizes["col"]),
        mesh=mesh,
        in_specs=(P(None, "row", "col"), P("row", "col")),
        out_specs=(P("row", "col"), P("row", "col"), P(None, "col"), P(None, "col")),
        check_vma=False,
    )
```

```python
import functools

import jax
import jax.numpy as jnp
from jax import lax
from jax.experimental import pallas as pl
from jax.experimental.pallas import tpu as pltpu
from jax.sharding import PartitionSpec as P

ITERS = 3
MESH = pl.DeviceIdType.MESH
HALO = 4
TOP = 16
SIDES = ((-1, 0), (1, 0), (0, -1), (0, 1), (-1, -1), (-1, 1), (1, -1), (1, 1))


def load_strip(ref, index, start, lanes):
    start = start if isinstance(start, int) else pl.multiple_of(start, 8)
    parts = [ref[index + (pl.ds(start, 8), pl.ds(first, size))] for first, size in lanes]
    return parts[0] if len(parts) == 1 else jnp.concatenate(parts, axis=1)


def neighbour_sum(ref, index, start, lanes, mid):
    width = mid.shape[1]
    above = load_strip(ref, index, start - 8, lanes)
    below = load_strip(ref, index, start + 8, lanes)
    sub = lax.broadcasted_iota(jnp.int32, mid.shape, 0)
    up = pltpu.roll(jnp.where(sub == 7, above, mid), 1, axis=0)
    down = pltpu.roll(jnp.where(sub == 0, below, mid), 7, axis=0)
    left = pltpu.roll(mid, 1, axis=1)
    right = pltpu.roll(mid, width - 1, axis=1)
    return (up + down) + (left + right)


def fold_lanes(strip, cols):
    total = strip[:, 0:128]
    for tile in range(1, cols // 128):
        total = total + strip[:, tile * 128:(tile + 1) * 128]
    return total


def quadratic(left, right, moments, shift):
    total = None
    for i, a in enumerate(left):
        for j, b in enumerate(right):
            term = a * b * moments[i + j + shift]
            total = term if total is None else total + term
    return total


def padded_sum(a, b):
    if len(a) < len(b):
        a, b = b, a
    return [x + b[i] if i < len(b) else x for i, x in enumerate(a)]


def coefficients(moments):
    residual = [jnp.ones_like(moments[0])]
    direction = residual
    solution_coords = [jnp.zeros_like(moments[0])]
    norm_now = moments[0]
    for iteration in range(ITERS):
        applied_dot = 4.0 * (
            quadratic(direction, direction, moments, 0)
            - quadratic(direction, direction, moments, 1)
        )
        step = norm_now / applied_dot
        solution_coords = padded_sum(solution_coords, [step * d for d in direction])
        if iteration + 1 < ITERS:
            moved = [-4.0 * step * d for d in direction]
            residual = padded_sum(residual, moved)
            residual = padded_sum(residual, [jnp.zeros_like(step)] + [-m for m in moved])
            norm_next = quadratic(residual, residual, moments, 0)
            ratio = norm_next / norm_now
            direction = padded_sum(residual, [ratio * d for d in direction])
            norm_now = norm_next
    return solution_coords


def pooled(values, half, slot, pool, stride):
    total = None
    for _ in range(3):
        piece = values.astype(jnp.bfloat16)
        values = values - piece.astype(jnp.float32)
        part = jnp.dot(piece, pool, preferred_element_type=jnp.float32)
        total = part if total is None else total + part
    lines = values.shape[0]
    half[slot, 0:lines, :] = total
    result = half[slot, pl.ds(0, lines // stride, stride=stride), :]
    for line in range(1, stride):
        result = result + half[slot, pl.ds(line, lines // stride, stride=stride), :]
    return result


def pool_matrix(stride):
    shape = (128 * stride, 128)
    source, target = (lax.broadcasted_iota(jnp.int32, shape, d) for d in range(2))
    return jnp.where(source // stride == target, 1.0 / (stride * stride), 0.0).astype(jnp.bfloat16)


def gather_kernel(
    n_row, n_col, rows, cols, kinds,
    src_hbm, lab_hbm, vec, mids, coord_ref,
    src, lab, mask, pack_r, pack_c, got_r, got_c, got_d, moment, half,
    load_sem, send_sem, recv_sem, mom_send, mom_recv, mid_send, mid_recv, fwd_send, fwd_recv,
):
    width = cols + 128
    n = n_row * n_col
    row, col = lax.axis_index("row"), lax.axis_index("col")
    me = row * n_col + col
    loads = [
        pltpu.make_async_copy(
            src_hbm.at[k], src.at[k, pl.ds(TOP, rows), pl.ds(0, cols)], load_sem.at[k]
        )
        for k in range(kinds)
    ]
    loads.append(
        pltpu.make_async_copy(lab_hbm, lab.at[pl.ds(TOP, rows), pl.ds(0, cols)], load_sem.at[kinds])
    )
    for load in loads:
        load.start()

    barrier = pltpu.get_barrier_semaphore()

    columns = [col]
    for _ in range(n_col - 1):
        columns.append(jnp.where(columns[-1] + 1 == n_col, 0, columns[-1] + 1))

    def for_all_others(act):
        for c in columns[1:]:
            act(row, c)

        def body(step, _):
            r = row + step
            r = jnp.where(r >= n_row, r - n_row, r)
            for c in columns:
                act(r, c)
            return 0

        lax.fori_loop(1, n_row, body, 0)

    for_all_others(lambda r, c: pl.semaphore_signal(
        barrier, inc=1, device_id=(r, c), device_id_type=MESH))

    first_row, last_row = row == 0, row == n_row - 1
    first_col, last_col = col == 0, col == n_col - 1
    quarter = jnp.full((8, width), 0.25, jnp.float32)
    lane = lax.broadcasted_iota(jnp.int32, (8, width), 1)
    off = ((lane >= cols) & (lane < cols + 64) & last_col) | ((lane >= cols + 64) & first_col)
    inside = jnp.where(off, 0.0, quarter)
    mask[0] = jnp.where(first_row, 0.0, inside)
    mask[1] = inside
    mask[2] = jnp.where(last_row, 0.0, inside)
    zero = jnp.zeros((8, width), jnp.float32)
    for which in range(3):
        vec[which, 0:8] = zero
        vec[which, rows + 24:rows + 32] = zero

    for load in loads:
        load.wait()

    for k in range(kinds + 1):
        def edge(rng, lanes):
            if k < kinds:
                return src[k, rng, lanes]
            return lab[rng, lanes].astype(jnp.float32)

        at = slice(HALO * k, HALO * (k + 1))
        pack_r[0, at, :] = edge(pl.ds(TOP, HALO), pl.ds(0, cols))
        pack_r[1, at, :] = edge(pl.ds(TOP + rows - HALO, HALO), pl.ds(0, cols))
    n_pack = HALO * (kinds + 1)
    tile_lane = lax.broadcasted_iota(jnp.int32, (rows, 128), 1)
    packed = jnp.zeros((rows, 128), jnp.float32)
    for k in range(kinds + 1):
        for side in range(2):
            lanes = pl.ds(0 if side == 0 else cols - 128, 128)
            if k < kinds:
                tile = src[k, pl.ds(TOP, rows), lanes]
            else:
                tile = lab[pl.ds(TOP, rows), lanes].astype(jnp.float32)
            target = side * n_pack + HALO * k
            origin = 0 if side == 0 else 128 - HALO
            if (target - origin) % 128:
                tile = pltpu.roll(tile, (target - origin) % 128, axis=1)
            packed = jnp.where((tile_lane >= target) & (tile_lane < target + HALO), tile, packed)
    turned = jnp.transpose(packed)
    pack_c[0] = turned[0:n_pack]
    pack_c[1] = turned[n_pack:2 * n_pack]

    groups = rows // 8 + 2
    whole = ((0, width),)
    around = ((cols - 128, 256), (0, 128))

    def right_side(start, lanes):
        here = load_strip(lab, (), start, lanes)
        total = jnp.zeros(here.shape, jnp.float32)
        for k in range(kinds):
            mid = load_strip(src, (k,), start, lanes)
            term = 4.0 * mid - neighbour_sum(src, (k,), start, lanes, mid)
            total = jnp.where(here == k, term, total)
        return total

    def stage(which, g, lanes, share):
        start = g * 8
        if which == 0:
            return right_side(start, lanes)
        mid = load_strip(vec, (which - 1,), start, lanes)
        return load_strip(mask, (share,), 0, lanes) * neighbour_sum(
            vec, (which - 1,), start, lanes, mid)

    def inner(which):
        def body(g, _):
            vec[which, pl.ds(pl.multiple_of(g * 8, 8), 8), :] = stage(which, g, whole, 1)
            return 0

        lax.fori_loop(2, groups, body, 0, unroll=2)

    edge_lane = lax.broadcasted_iota(jnp.int32, (8, 128), 1)

    def frame(which):
        for g, share in ((1, 0), (2, 1), (groups - 1, 1), (groups, 2)):
            vec[which, pl.ds(g * 8, 8), :] = stage(which, g, whole, share)

        def body(g, _):
            lines = pl.ds(pl.multiple_of(g * 8, 8), 8)
            new = stage(which, g, around, 1)
            last = vec[which, lines, pl.ds(cols - 128, 128)]
            first = vec[which, lines, pl.ds(0, 128)]
            vec[which, lines, pl.ds(cols - 128, 128)] = jnp.where(
                edge_lane >= 64, new[:, 0:128], last)
            vec[which, lines, pl.ds(cols, 128)] = new[:, 128:256]
            vec[which, lines, pl.ds(0, 128)] = jnp.where(edge_lane < 64, new[:, 256:384], first)
            return 0

        lax.fori_loop(3, groups - 1, body, 0, unroll=2)

    inner(0)
    pl.semaphore_wait(barrier, n - 1)

    sends = []
    for i, (dr, dc) in enumerate(SIDES):
        if dc == 0:
            source = pack_r.at[0 if dr < 0 else 1]
            target = got_r.at[1 if dr < 0 else 0]
        elif dr == 0:
            source = pack_c.at[0 if dc < 0 else 1]
            target = got_c.at[1 if dc < 0 else 0]
        else:
            lanes = pl.ds(0 if dc < 0 else cols - 128, 128)
            source = pack_r.at[0 if dr < 0 else 1, :, lanes]
            target = got_d.at[1 if dr < 0 else 0, 1 if dc < 0 else 0]
        there = jnp.logical_and(
            jnp.logical_and(row + dr >= 0, row + dr < n_row),
            jnp.logical_and(col + dc >= 0, col + dc < n_col),
        )
        opposite = SIDES.index((-dr, -dc))
        device = (
            jnp.clip(row + dr, 0, n_row - 1),
            jnp.clip(col + dc, 0, n_col - 1),
        )
        copy = pltpu.make_async_remote_copy(
            src_ref=source, dst_ref=target, send_sem=send_sem.at[i],
            recv_sem=recv_sem.at[opposite], device_id=device, device_id_type=MESH,
        )
        back = pltpu.make_async_remote_copy(
            src_ref=source, dst_ref=got_r.at[0 if dr < 0 else 1] if dc == 0 else (
                got_c.at[0 if dc < 0 else 1] if dr == 0
                else got_d.at[0 if dr < 0 else 1, 0 if dc < 0 else 1]),
            send_sem=send_sem.at[i], recv_sem=recv_sem.at[i],
            device_id=device, device_id_type=MESH,
        )
        sends.append((there, copy, back))
        pl.when(there)(copy.start)
    for which in range(1, ITERS):
        inner(which)

    for there, copy, back in sends:
        pl.when(there)(back.wait_recv)

    halo_lane = lax.broadcasted_iota(jnp.int32, (HALO, 128), 1)
    for side in range(2):
        missing_row = first_row if side == 0 else last_row
        base = TOP - HALO if side == 0 else TOP + rows
        other = TOP - 8 if side == 0 else TOP + rows + HALO
        for k in range(kinds + 1):
            fill = jnp.float32(0.0 if k < kinds else -1.0)
            at = slice(HALO * k, HALO * (k + 1))
            wide = jnp.where(missing_row, fill, got_r[side, at, :])
            right = jnp.where(
                (halo_lane < HALO) & jnp.logical_not(missing_row | last_col),
                got_d[side, 1, at, :], fill)
            corner = jnp.where(
                (halo_lane >= 128 - HALO) & jnp.logical_not(missing_row | first_col),
                got_d[side, 0, at, :], right)
            empty = jnp.full((HALO, width), fill)
            if k < kinds:
                src[k, pl.ds(base, HALO), pl.ds(0, cols)] = wide
                src[k, pl.ds(base, HALO), pl.ds(cols, 128)] = corner
                src[k, pl.ds(other, HALO), :] = empty
            else:
                lab[pl.ds(base, HALO), pl.ds(0, cols)] = wide.astype(jnp.int32)
                lab[pl.ds(base, HALO), pl.ds(cols, 128)] = corner.astype(jnp.int32)
                lab[pl.ds(other, HALO), :] = empty.astype(jnp.int32)
    both = jnp.concatenate(
        [
            got_c[1],
            got_c[0],
            jnp.zeros((128 - 2 * n_pack, rows), jnp.float32),
        ],
        axis=0,
    )
    unturned = jnp.transpose(both)
    for k in range(kinds + 1):
        fill = jnp.float32(0.0 if k < kinds else -1.0)
        right = pltpu.roll(unturned, (-HALO * k) % 128, axis=1)
        left = pltpu.roll(unturned, (128 - HALO - n_pack - HALO * k) % 128, axis=1)
        tile = jnp.where((tile_lane < HALO) & jnp.logical_not(last_col), right, fill)
        tile = jnp.where((tile_lane >= 128 - HALO) & jnp.logical_not(first_col), left, tile)
        if k < kinds:
            src[k, pl.ds(TOP, rows), pl.ds(cols, 128)] = tile
        else:
            lab[pl.ds(TOP, rows), pl.ds(cols, 128)] = tile.astype(jnp.int32)

    chips = n_row // 2
    partner = row + 1 - 2 * lax.rem(row, 2)
    quad = rows // 4
    pool = pool_matrix(4)

    def block(w, owner):
        return mids.at[w, pl.ds(pl.multiple_of(owner * quad, 8), quad)]

    def peer(step):
        other = row + 2 * step
        return jnp.where(other >= n_row, other - n_row, other)

    def hand(w, owner, target, send, recv):
        return pltpu.make_async_remote_copy(
            src_ref=block(w, owner), dst_ref=block(w, owner), send_sem=send, recv_sem=recv,
            device_id=(target, col), device_id_type=MESH)

    def gather(w):
        for tile in range(cols // 512):
            mids[w, pl.ds(pl.multiple_of(row * quad, 8), quad), pl.ds(tile * 128, 128)] = pooled(
                vec[w, pl.ds(TOP, rows), pl.ds(tile * 512, 512)], half,
                w * (cols // 512) + tile, pool, 4)
        hops = [
            hand(w, row, peer(step), mid_send.at[w, step], mid_recv.at[w, step])
            for step in range(1, chips)
        ]
        hops.append(hand(w, row, partner, mid_send.at[w, 0], mid_recv.at[w, 0]))
        for hop in hops:
            hop.start()
        return hops

    hops = []
    frame(0)
    for which in range(ITERS - 1):
        hops += gather(which)
        frame(which + 1)

    def products(g, sums):
        start = pl.multiple_of(g * 8, 8)
        powers = [vec[w, pl.ds(start, 8), :] for w in range(ITERS)]
        powers.append(0.25 * neighbour_sum(vec, (ITERS - 1,), start, whole, powers[-1]))
        return tuple(
            s + fold_lanes(powers[i // 2] * powers[(i + 1) // 2], cols)
            for i, s in enumerate(sums)
        )

    sums = lax.fori_loop(
        2, groups, products, tuple(jnp.zeros((8, 128), jnp.float32) for _ in range(2 * ITERS)), unroll=2)
    lane1 = lax.broadcasted_iota(jnp.int32, (1, 128), 1)
    mine = jnp.zeros((1, 128), jnp.float32)
    for i, s in enumerate(sums):
        mine = jnp.where(lane1 == i, jnp.sum(s, keepdims=True), mine)
    moment[me] = mine

    for_all_others(lambda r, c: pltpu.make_async_remote_copy(
        src_ref=moment.at[me], dst_ref=moment.at[me], send_sem=mom_send, recv_sem=mom_recv,
        device_id=(r, c), device_id_type=MESH).start())
    hops += gather(ITERS - 1)
    everyone = moment.at[pl.ds(0, n - 1)]
    pltpu.make_async_copy(everyone, everyone, mom_recv).wait()
    total = jnp.sum(moment[...], axis=0)
    moments = [
        jnp.sum(jnp.where(lane1 == i, total, 0.0), axis=1, keepdims=True) for i in range(2 * ITERS)
    ]
    for w, c in enumerate(coefficients(moments)):
        coord_ref[w] = jnp.broadcast_to(c, (8, 128))

    def source_of(step):
        other = row - 2 * step
        return jnp.where(other < 0, other + n_row, other)

    def other_core(owner):
        return owner + 1 - 2 * lax.rem(owner, 2)

    forwards = []
    for w in range(ITERS):
        for step in range(1, chips):
            owner = source_of(step)
            hand(w, owner, partner, mid_send.at[w, step], mid_recv.at[w, step]).wait_recv()
            forward = hand(w, owner, partner, fwd_send.at[w, step], fwd_recv.at[w, step])
            forward.start()
            forwards.append(forward)
    for w in range(ITERS):
        hand(w, partner, partner, mid_send.at[w, 0], mid_recv.at[w, 0]).wait_recv()
        for step in range(1, chips):
            hand(w, other_core(source_of(step)), partner,
                 fwd_send.at[w, step], fwd_recv.at[w, step]).wait_recv()
    for hop in hops:
        hop.wait_send()
    for forward in forwards:
        forward.wait_send()
    for there, copy, back in sends:
        pl.when(there)(copy.wait_send)
    pltpu.make_async_copy(everyone, everyone, mom_send).wait()


def finish_kernel(
    rows, cols, vec, mids, coord_ref, blend_out, fine_out, mid_out, coarse_out,
    blend, fine, mid, coarse, half, out_sem,
):
    pool = pool_matrix(2)

    def leave(slot, source, target):
        copy = pltpu.make_async_copy(source, target, out_sem.at[slot])
        copy.start()
        return copy

    def combine(source, target, lines, lanes, first):
        coords = [jnp.concatenate([coord_ref[w]] * (lanes // 128), axis=1) for w in range(ITERS)]

        def body(g, _):
            start = pl.multiple_of(g * 8, 8)
            strip = None
            for w in range(ITERS):
                term = coords[w] * source[w, pl.ds(start + first, 8), pl.ds(0, lanes)]
                strip = term if strip is None else strip + term
            target[pl.ds(start, 8), :] = strip
            return 0

        lax.fori_loop(0, lines // 8, body, 0, unroll=4)

    combine(vec, blend, rows, cols, TOP)
    copies = [leave(0, blend, blend_out)]
    tall, wide = mid.shape
    combine(mids, mid, tall, wide, 0)
    copies.append(leave(1, mid, mid_out))
    for tile in range(cols // 256):
        fine[:, tile * 128:(tile + 1) * 128] = pooled(
            blend[:, tile * 256:(tile + 1) * 256], half, tile, pool, 2)
    copies.append(leave(2, fine, fine_out))
    for tile in range(wide // 256):
        coarse[:, tile * 128:(tile + 1) * 128] = pooled(
            mid[:, tile * 256:(tile + 1) * 256], half, cols // 256 + tile, pool, 2)
    copies.append(leave(3, coarse, coarse_out))
    for copy in copies:
        copy.wait()


def per_device(n_row, n_col, sources, labels):
    kinds, rows, cols = sources.shape
    n = n_row * n_col
    tall, width = rows + 32, cols + 128
    n_pack = HALO * (kinds + 1)
    f32 = jnp.float32
    vmem = pl.BlockSpec(memory_space=pltpu.VMEM)
    hbm = pl.BlockSpec(memory_space=pltpu.HBM)
    mid_shape = (n_row * rows // 4, cols // 4)
    coarse_shape = (n_row * rows // 8, cols // 8)
    chips = n_row // 2
    dma = pltpu.SemaphoreType.DMA
    vec, mids, coords = pl.pallas_call(
        functools.partial(gather_kernel, n_row, n_col, rows, cols, kinds),
        out_shape=(
            jax.ShapeDtypeStruct((ITERS, tall, width), f32),
            jax.ShapeDtypeStruct((ITERS,) + mid_shape, f32),
            jax.ShapeDtypeStruct((ITERS, 8, 128), f32),
        ),
        in_specs=[hbm] * 2,
        out_specs=(vmem,) * 3,
        scratch_shapes=[
            pltpu.VMEM((kinds, tall, width), f32),
            pltpu.VMEM((tall, width), jnp.int32),
            pltpu.VMEM((3, 8, width), f32),
            pltpu.VMEM((2, n_pack, cols), f32),
            pltpu.VMEM((2, n_pack, rows), f32),
            pltpu.VMEM((2, n_pack, cols), f32),
            pltpu.VMEM((2, n_pack, rows), f32),
            pltpu.VMEM((2, 2, n_pack, 128), f32),
            pltpu.VMEM((n, 1, 128), f32),
            pltpu.VMEM((ITERS * (cols // 512), rows, 128), f32),
            dma((kinds + 1,)),
            dma((8,)),
            dma((8,)),
            dma,
            dma,
            dma((ITERS, chips)),
            dma((ITERS, chips)),
            dma((ITERS, chips)),
            dma((ITERS, chips)),
        ],
        compiler_params=pltpu.CompilerParams(
            collective_id=0, has_side_effects=True, vmem_limit_bytes=20 * 2**20),
    )(
        pltpu.with_memory_space_constraint(sources, pltpu.HBM),
        pltpu.with_memory_space_constraint(labels, pltpu.HBM),
    )
    return pl.pallas_call(
        functools.partial(finish_kernel, rows, cols),
        out_shape=(
            jax.ShapeDtypeStruct((rows, cols), f32),
            jax.ShapeDtypeStruct((rows // 2, cols // 2), f32),
            jax.ShapeDtypeStruct(mid_shape, f32),
            jax.ShapeDtypeStruct(coarse_shape, f32),
        ),
        in_specs=[vmem] * 3,
        out_specs=(hbm,) * 4,
        scratch_shapes=[
            pltpu.VMEM((rows, cols), f32),
            pltpu.VMEM((rows // 2, cols // 2), f32),
            pltpu.VMEM(mid_shape, f32),
            pltpu.VMEM(coarse_shape, f32),
            pltpu.VMEM((cols // 256 + cols // 1024, max(rows, mid_shape[0]), 128), f32),
            dma((4,)),
        ],
        compiler_params=pltpu.CompilerParams(vmem_limit_bytes=20 * 2**20),
    )(vec, mids, coords)


def solution(mesh):
    sizes = dict(mesh.shape)
    return jax.shard_map(
        functools.partial(per_device, sizes["row"], sizes["col"]),
        mesh=mesh,
        in_specs=(P(None, "row", "col"), P("row", "col")),
        out_specs=(P("row", "col"), P("row", "col"), P(None, "col"), P(None, "col")),
        check_vma=False,
    )
```
